256 devices in a mesh: gx: 8 (over x, z_lo), gy: 8 (over z_hi, core), gz: 4 (over y).
Axes of the slice: x: 4, y: 4, z: 8 (z_hi: 4, z_lo: 2; z = z_hi * 2 + z_lo), core: 2. Of those that a mesh axis runs over, the one named last changes fastest.
Arguments:
- partials: float32 [32, 128, 128, 512], P('gx', None, 'gy', 'gz'), may hold values from -40 to 40
- code_bits: int32 [32, 128], replicated, may hold values from 0 to 1
- group_map: int32 [32], replicated, may hold values from 0 to 31, each once
- velocity: float32 [128, 128, 512], P('gx', 'gy', 'gz'), may hold values from 1.5 to 4.5
Outputs:
- gradient: float32 [128, 128, 512], P('gx', 'gy', 'gz')
- new_model: float32 [128, 128, 512], P('gx', 'gy', 'gz')
The draws below stay inside these ranges and needn't reach their ends.
Inputs may be any that keep to these rules, and one draw needn't show every extreme that they name: `group_map`: every group of 0 to 31 stands in exactly one slot.
All inputs are finite; a program needn't handle non-finite values.
Results may differ from the reference program's by a relative error of at most 0.0001.
Values sent between devices are 32-bit elements; how exact they have to be, the bound alone decides.
A program may use at most 64 MiB of HBM per device.

```python
import jax
import jax.numpy as jnp
from jax import lax

G = 32
ITERS = 3
NX = 128
NY = 128
NZ = 512


def draw_partials(key, part):
    first_key = jax.random.fold_in(jax.random.fold_in(key, 17), 0)
    rough = jnp.clip(jax.random.normal(first_key, (G, NX, NY, NZ), jnp.float32), -6.0, 6.0)
    return rough


def set_ends(result, rng, smallest, top_value):
    longest = result.shape.index(max(result.shape))
    spots = []
    for shift in (0, 1):
        where = [jax.random.randint(jax.random.fold_in(rng, axis), (), 0, length) for axis, length in enumerate(result.shape)]
        where[longest] = (where[longest] + shift) % result.shape[longest]
        spots.append(tuple(where))
    return result.at[spots[0]].set(smallest).at[spots[1]].set(top_value)


def block_scale(key, dims, pieces, low, top_value):
    def one(axis_at, parts):
        draws = jax.random.uniform(jax.random.fold_in(jax.random.fold_in(key, 6), axis_at), (parts,), jnp.float32, low / len(pieces), top_value / len(pieces))
        return jnp.repeat(jnp.exp(draws), dims[axis_at] // parts).reshape((-1,) + (1,) * (len(dims) - axis_at - 1))

    loudness = one(*pieces[0])
    for cut in pieces[1:]:
        loudness = loudness * one(*cut)
    return loudness


def setup_inputs(seed: int = 0) -> dict:
    arg_keys = jax.random.split(jax.random.key(seed), 5)
    return {
        "partials": draw_partials(jax.random.fold_in(arg_keys[4], 71), 0),
        "code_bits": set_ends(jax.random.randint(arg_keys[1], (G, NX), 0, 2), jax.random.fold_in(arg_keys[1], 1), 0, 1).astype(jnp.int32),
        "group_map": jax.random.permutation(arg_keys[2], G).astype(jnp.int32),
        "velocity": jnp.clip(1.5 + 3.0 * jax.random.uniform(arg_keys[3], (NX, NY, NZ), jnp.float32) ** block_scale(arg_keys[3], (NX, NY, NZ), ((0, 8), (1, 8), (2, 4)), -0.2, 0.2), 1.5, 4.5),
    }


step_length = 0.5
tv_weight = 0.2
dual_step = 0.28
primal_step = 0.28

def forward_diff(field):
    zeros_x = jnp.zeros((1,) + field.shape[1:], jnp.float32)
    zeros_y = jnp.zeros((field.shape[0], 1, field.shape[2]), jnp.float32)
    zeros_z = jnp.zeros(field.shape[:2] + (1,), jnp.float32)
    diff_x = jnp.concatenate([field[1:] - field[:-1], zeros_x], 0)
    diff_y = jnp.concatenate([field[:, 1:] - field[:, :-1], zeros_y], 1)
    diff_z = jnp.concatenate([field[:, :, 1:] - field[:, :, :-1], zeros_z], 2)
    return jnp.stack([diff_x, diff_y, diff_z])

def divergence(dual_field):
    left_x = jnp.pad(dual_field[0][:-1], ((1, 0), (0, 0), (0, 0)))
    left_y = jnp.pad(dual_field[1][:, :-1], ((0, 0), (1, 0), (0, 0)))
    left_z = jnp.pad(dual_field[2][:, :, :-1], ((0, 0), (0, 0), (1, 0)))
    return dual_field[0] - left_x + (dual_field[1] - left_y) + (dual_field[2] - left_z)

def reference(partials, code_bits, group_map, velocity):
    sign_table = 2.0 * code_bits[group_map].astype(jnp.float32) - 1.0

    def accumulate(index, acc):
        return acc + sign_table[index][:, None, None] * partials[index]
    gradient = lax.fori_loop(0, partials.shape[0], accumulate, jnp.zeros(velocity.shape, jnp.float32))
    mean_square = jnp.sum(gradient * gradient) / gradient.size
    step_scale = step_length / jnp.sqrt(mean_square + 1.0)
    target = velocity - step_scale * gradient
    current = target
    extra = target
    dual_field = jnp.zeros((3,) + target.shape, jnp.float32)
    for iteration in range(ITERS):
        dual_field = dual_field + dual_step * forward_diff(extra)
        magnitude = jnp.sqrt(lax.optimization_barrier(jnp.sum(dual_field * dual_field, axis=0)))
        dual_field = dual_field / jnp.maximum(1.0, magnitude / tv_weight)[None]
        updated = (current + primal_step * divergence(dual_field) + primal_step * target) / (1.0 + primal_step)
        extra = 2.0 * updated - current
        current = updated
    return (gradient, current)
```

```python
import functools

import jax
import jax.numpy as jnp
from jax import lax
from jax.experimental import pallas as pl
from jax.experimental.pallas import tpu as pltpu
from jax.sharding import PartitionSpec as P

ITERS = 3
H = ITERS
SEG = 16
PARTS = ((2, 6, 1), (6, 1, 2), (1, 2, 6))
LOAD_ORDER = (5, 4, 7, 3, 2, 6, 1, 0)

step_length = 0.5
tv_weight = 0.2
dual_step = 0.28
primal_step = 0.28
MESH = pl.DeviceIdType.MESH


def geometry(dims):
    nx, ny, nz, slots, bx, by, bz = dims
    win = bx + H * min(2, nx - 1)
    tiles = -(-win // (bz // SEG))
    yp = -(-(by + 2 * H) // 8) * 8
    return win, tiles, yp, 16 + (win + tiles) * yp


def own_offset(nx, bx, win, q):
    if nx == 1:
        return 0
    return jnp.where(q == 0, 0, jnp.where(q == nx - 1, win - bx, H))


def roll(value, shift):
    shift = shift % value.shape[1]
    return value if shift == 0 else pltpu.roll(value, shift, 1)


def xor_masks(ix):
    two = ix + 2 - 4 * lax.rem(lax.div(ix, 2), 2)
    six = 6 - 2 * lax.div(ix, 2) + lax.rem(ix, 2)
    four = lax.rem(ix + 4, 8)
    flip = lambda q: q + 1 - 2 * lax.rem(q, 2)
    return {
        0: ix, 1: flip(ix), 2: two, 3: flip(two),
        4: four, 5: flip(four), 6: six, 7: flip(six),
    }


def kernel(
    dims,
    partials,
    code_bits,
    group_map,
    velocity,
    va,
    ga,
    gw,
    scale_out,
    bits,
    gmap,
    part,
    psum,
    vw,
    r1,
    r2,
    r3,
    s2,
    s3,
    ys,
    yr,
    ss,
    zr,
    ds,
    dr,
    za,
    ara,
    arb,
    in_sem,
    part_sem,
    s1_sems,
    r1_sems,
    s2_sems,
    r2_sems,
    s3_sems,
    r3_sems,
    xs_sem,
    xr_sem,
    hs_sem,
    hr_sem,
    as_sem,
    ar_sem,
    bs_sem,
    br_sem,
):
    nx, ny, nz, slots, bx, by, bz = dims
    win, tiles, yp, flat = geometry(dims)
    groups = bz // SEG
    ix, iy, iz = lax.axis_index("gx"), lax.axis_index("gy"), lax.axis_index("gz")
    xi, zl = lax.div(ix, 2), lax.rem(ix, 2)
    offset = functools.partial(own_offset, nx, bx, win)
    off = offset(ix)
    block = xor_masks(ix)
    per = bx * by // 8

    in_copies = [
        pltpu.make_async_copy(code_bits, bits, in_sem.at[0]),
        pltpu.make_async_copy(group_map, gmap, in_sem.at[1]),
    ]
    v_copy = pltpu.make_async_copy(velocity, vw.at[pl.ds(off, bx)], in_sem.at[2])
    for c in in_copies:
        c.start()
    part_copies = {}
    for mask in LOAD_ORDER:
        where = pl.ds(block[mask] * bx, bx)
        part_copies[mask] = pltpu.make_async_copy(
            partials.at[:, where], part.at[:, where], part_sem.at[mask]
        )
        part_copies[mask].start()
    v_copy.start()

    barrier = pltpu.get_barrier_semaphore()

    def at(x=None, y=None, z=None):
        return (ix if x is None else x, iy if y is None else y, iz if z is None else z)

    def notify(sem, device):
        pl.semaphore_signal(sem, inc=1, device_id=device, device_id_type=MESH)

    for buffer in (yr, zr, dr):
        buffer[...] = jnp.zeros_like(buffer)

    ring = lambda d, n: min(d, n - d)
    plane = [(dx, dz) for dx in range(4) for dz in range(nz) if dx or dz]
    plane.sort(key=lambda p: -(ring(p[0], 4) + ring(p[1], nz)))
    stack = [(dl, dy) for dl in range(2) for dy in range(ny) if dl or dy]
    stack.sort(key=lambda p: -(p[0] + 2 * ring(p[1] // 2, max(ny // 2, 1)) + p[1] % 2))

    def plane_device(dx, dz):
        return at(x=2 * lax.rem(xi + dx, 4) + zl, z=lax.rem(iz + dz, nz))

    def stack_device(dl, dy):
        return at(x=2 * xi + lax.rem(zl + dl, 2), y=lax.rem(iy + dy, ny))

    has = {
        "y-": iy > 0,
        "y+": iy < ny - 1,
        "z-": iz > 0,
        "z+": iz < nz - 1,
    }
    near = {
        "y-": at(y=iy - 1),
        "y+": at(y=iy + 1),
        "z-": at(z=iz - 1),
        "z+": at(z=iz + 1),
    }
    both = lambda a, b: jnp.logical_and(has[a], has[b])
    for p in plane:
        notify(barrier, plane_device(*p))
    for p in stack:
        notify(barrier, stack_device(*p))
    total = jnp.int32(len(plane) + len(stack))
    extra = [
        (both("y+", "z+"), at(y=iy + 1, z=iz + 1)),
        (both("y+", "z-"), at(y=iy + 1, z=iz - 1)),
        (both("y-", "z+"), at(y=iy - 1, z=iz + 1)),
        (both("y-", "z-"), at(y=iy - 1, z=iz - 1)),
        (jnp.logical_and(zl == 1, ix < nx - 1), at(x=ix + 1)),
        (jnp.logical_and(zl == 0, ix > 0), at(x=ix - 1)),
    ]
    for present, device in extra:
        total = total + present.astype(jnp.int32)

        @pl.when(present)
        def _(device=device):
            notify(barrier, device)

    for buffer in (za, va, ga):
        buffer[...] = jnp.zeros_like(buffer)

    def x_halo(buffer, f, side):
        q = ix + 1 if side == 0 else ix - 1
        src = off + bx - H if side == 0 else off
        dst = offset(q) - H if side == 0 else offset(q) + bx
        return pltpu.make_async_remote_copy(
            src_ref=buffer.at[pl.ds(src, H)],
            dst_ref=buffer.at[pl.ds(dst, H)],
            send_sem=xs_sem.at[f, side],
            recv_sem=xr_sem.at[f, side],
            device_id=at(x=q),
            device_id_type=MESH,
        )

    def x_send(buffer, f):
        pl.when(ix < nx - 1)(x_halo(buffer, f, 0).start)
        pl.when(ix > 0)(x_halo(buffer, f, 1).start)

    def x_arrive(buffer, f):
        for side in range(2):
            zone = buffer.at[pl.ds(off - H if side == 0 else off + bx, H)]
            arrived = pltpu.make_async_copy(zone, zone, xr_sem.at[f, side])
            pl.when(ix > 0 if side == 0 else ix < nx - 1)(arrived.wait)

    for c in in_copies:
        c.wait()
    codes = [gmap[ix * slots + s] for s in range(slots)]

    def reduce_block(mask):
        part_copies[mask].wait()
        first = block[mask] * bx

        def one(r, carry):
            row = first + r
            acc = None
            for s in range(slots):
                sign = (2 * bits[codes[s], row] - 1).astype(jnp.float32)
                term = sign * part[s, row]
                acc = term if acc is None else acc + term
            for h in range(by // 8):
                psum[row * (by // 8) + h] = acc[8 * h : 8 * h + 8]
            return carry

        lax.fori_loop(0, bx, one, 0, unroll=4)

    cuts = [per * k // 3 for k in range(4)]

    def span(mask, k):
        return pl.ds(block[mask] * per + cuts[k], cuts[k + 1] - cuts[k])

    def hop(k, step, m, src):
        width = cuts[k + 1] - cuts[k]
        to = r1.at[k, m] if step == 0 else r2.at[k, m] if step == 1 else r3.at[k]
        sends = s1_sems.at[k, m] if step == 0 else s2_sems.at[k, m] if step == 1 else s3_sems.at[k]
        recvs = r1_sems.at[k, m] if step == 0 else r2_sems.at[k, m] if step == 1 else r3_sems.at[k]
        return pltpu.make_async_remote_copy(
            src_ref=src,
            dst_ref=to.at[pl.ds(0, width)],
            send_sem=sends,
            recv_sem=recvs,
            device_id=at(x=block[PARTS[k][step]]),
            device_id_type=MESH,
        )

    def kept(k):
        a, b, c = PARTS[k]
        return [b ^ c, b, c, 0]

    def first_hop(k, m):
        return hop(k, 0, m, psum.at[span(PARTS[k][0] ^ kept(k)[m], k)])

    def second_hop(k, m):
        return hop(k, 1, m, s2.at[k, m, pl.ds(0, cuts[k + 1] - cuts[k])])

    def third_hop(k):
        return hop(k, 2, 0, s3.at[k, pl.ds(0, cuts[k + 1] - cuts[k])])

    done = set()
    for m in range(4):
        for k in range(3):
            mask = PARTS[k][0] ^ kept(k)[m]
            if mask not in done:
                done.add(mask)
                reduce_block(mask)
                if len(done) == 1:
                    pl.semaphore_wait(barrier, total)
            first_hop(k, m).start()
    reduce_block(0)
    v_copy.wait()
    x_send(vw, 0)

    lane = lax.broadcasted_iota(jnp.int32, (1, bz), 1)
    group = lane // SEG
    spot = lax.rem(lane, SEG)

    def pack(read, k):
        acc = None
        for g in range(groups):
            x = tiles * g + k
            if x >= win:
                continue
            moved = roll(read(x), H + SEG * g)
            acc = moved if acc is None else jnp.where(group == g, moved, acc)
        return acc

    def prepare(f, field):
        for x in range(win):
            tile = field[x]
            ys[0, f, x * H : x * H + H] = tile[by - H : by]
            ys[1, f, x * H : x * H + H] = tile[0:H]
        for k in range(tiles):
            tile = pack(lambda x: field[x], k)
            ss[f, k] = tile
            ds[0, f, k * H : k * H + H] = tile[by - H : by]
            ds[1, f, k * H : k * H + H] = tile[0:H]

    def exchange(f):
        def send(src, dst, n, device):
            return pltpu.make_async_remote_copy(
                src_ref=src.at[f],
                dst_ref=dst.at[f],
                send_sem=hs_sem.at[f, n],
                recv_sem=hr_sem.at[f, n],
                device_id=device,
                device_id_type=MESH,
            )

        up, down = ds.at[0], ds.at[1]
        pp, pm = both("y+", "z+"), both("y+", "z-")
        mp, mm = both("y-", "z+"), both("y-", "z-")
        return [
            (send(ys.at[0], yr.at[0], 0, near["y+"]), has["y+"], has["y-"]),
            (send(ys.at[1], yr.at[1], 1, near["y-"]), has["y-"], has["y+"]),
            (send(ss, zr.at[0], 2, near["z+"]), has["z+"], has["z-"]),
            (send(ss, zr.at[1], 3, near["z-"]), has["z-"], has["z+"]),
            (send(up, dr.at[0], 4, at(y=iy + 1, z=iz + 1)), pp, mm),
            (send(up, dr.at[1], 5, at(y=iy + 1, z=iz - 1)), pm, mp),
            (send(down, dr.at[2], 6, at(y=iy - 1, z=iz + 1)), mp, pm),
            (send(down, dr.at[3], 7, at(y=iy - 1, z=iz - 1)), mm, pp),
        ]

    def send_all(f):
        for copy, sends, _ in exchange(f):
            pl.when(sends)(copy.start)

    def receive_all(f):
        for copy, _, receives in exchange(f):
            pl.when(receives)(copy.wait_recv)

    front = 8

    def base(x):
        return front + x * yp

    def assemble(f, field, whole):
        for x in range(win):
            b = base(x)
            whole[b + H : b + H + by] = field[x]
            whole[b : b + H] = yr[0, f, x * H : x * H + H]
            whole[b + H + by : b + 2 * H + by] = yr[1, f, x * H : x * H + H]
        for k in range(tiles):
            for z in range(2):
                za[z, H : H + by] = zr[z, f, k]
                za[z, 0:H] = dr[z, f, k * H : k * H + H]
                za[z, H + by : 2 * H + by] = dr[2 + z, f, k * H : k * H + H]
            left = za[0, 0:yp]
            mine = pack(lambda x: whole[base(x) : base(x) + yp], k)
            right = roll(za[1, 0:yp], SEG // 2)
            b = base(win + k)
            whole[b : b + yp] = jnp.where(
                spot < H,
                left,
                jnp.where(
                    spot < SEG // 2,
                    mine,
                    jnp.where(spot < SEG // 2 + H, roll(mine, SEG // 2), right),
                ),
            )

    for m in range(2):
        for k in range(3):
            first_hop(k, m).wait_recv()
            width = cuts[k + 1] - cuts[k]
            s2[k, m, 0:width] = psum[span(kept(k)[m], k)] + r1[k, m, 0:width]
            second_hop(k, m).start()

    x_arrive(vw, 0)
    prepare(0, vw)
    send_all(0)

    for k in range(3):
        first_hop(k, 2).wait_recv()
        second_hop(k, 0).wait_recv()
        width = cuts[k + 1] - cuts[k]
        mine = psum[span(kept(k)[2], k)] + r1[k, 2, 0:width]
        s3[k, 0:width] = mine + r2[k, 0, 0:width]
        third_hop(k).start()

    squares = jnp.zeros((8, bz), jnp.float32)
    for k in range(3):
        first_hop(k, 3).wait_recv()
        second_hop(k, 1).wait_recv()
        third_hop(k).wait_recv()
        for j in range(cuts[k], cuts[k + 1]):
            n = j - cuts[k]
            value = psum[ix * per + j] + r1[k, 3, n] + (r2[k, 1, n] + r3[k, n])
            r, h = divmod(j, by // 8)
            gw[off + r, 8 * h : 8 * h + 8] = value
            squares = squares + value * value

    def spread(buffer, me, peers, device, send_sem, recv_sem):
        for p in peers:
            pltpu.make_async_remote_copy(
                src_ref=buffer.at[me],
                dst_ref=buffer.at[me],
                send_sem=send_sem,
                recv_sem=recv_sem,
                device_id=device(*p),
                device_id_type=MESH,
            ).start()

    def drain(buffer, peers, sem):
        many = buffer.at[pl.ds(0, len(peers))]
        pltpu.make_async_copy(many, many, sem).wait()

    me_a = xi * nz + iz
    ara[me_a] = jnp.sum(squares, axis=0, keepdims=True)
    spread(ara, me_a, plane, plane_device, as_sem, ar_sem)
    x_send(gw, 1)
    receive_all(0)
    assemble(0, vw, va)
    for k in range(3):
        for m in range(4):
            first_hop(k, m).wait_send()
        for m in range(2):
            second_hop(k, m).wait_send()
        third_hop(k).wait_send()
    x_arrive(gw, 1)
    prepare(1, gw)
    send_all(1)

    drain(ara, plane, ar_sem)
    me_b = zl * ny + iy
    arb[me_b] = jnp.sum(ara[...], axis=0)
    spread(arb, me_b, stack, stack_device, bs_sem, br_sem)

    receive_all(1)
    assemble(1, gw, ga)
    drain(ara, plane, as_sem)
    for f, buffer in ((0, vw), (1, gw)):
        pl.when(ix < nx - 1)(x_halo(buffer, f, 0).wait_send)
        pl.when(ix > 0)(x_halo(buffer, f, 1).wait_send)
        for copy, sends, _ in exchange(f):
            pl.when(sends)(copy.wait_send)

    drain(arb, stack, br_sem)
    square_sum = jnp.sum(jnp.sum(arb[...], axis=0), axis=1, keepdims=True)
    cells = nx * ny * nz * bx * by * bz
    scale = step_length * lax.rsqrt(square_sum / cells + 1.0)
    scale_out[...] = jnp.broadcast_to(scale, scale_out.shape)
    drain(arb, stack, bs_sem)


def proximal(
    dims,
    va,
    ga,
    gw,
    scale_in,
    gradient_out,
    model_out,
    target,
    current,
    extra,
    dx,
    dy,
    dz,
    result,
    out_sem,
):
    nx, ny, nz, slots, bx, by, bz = dims
    win, tiles, yp, flat = geometry(dims)
    ix, iy, iz = lax.axis_index("gx"), lax.axis_index("gy"), lax.axis_index("gz")
    off = own_offset(nx, bx, win, ix)
    g_out = pltpu.make_async_copy(gw.at[pl.ds(off, bx)], gradient_out, out_sem.at[0])
    g_out.start()
    front = 8

    def base(x):
        return front + x * yp

    edge_rows = jnp.zeros((front, bz), jnp.float32)
    dy[0:front] = edge_rows
    target[flat - front : flat] = edge_rows
    extra[flat - front : flat] = edge_rows
    scale = scale_in[...]
    lane = lax.broadcasted_iota(jnp.int32, (1, bz), 1)
    group = lane // SEG
    spot = lax.rem(lane, SEG)
    y_at = iy * by - H + lax.broadcasted_iota(jnp.int32, (yp, 1), 0)
    keep_y = jnp.logical_and(y_at >= 0, y_at < ny * by - 1)
    keep_y = jnp.broadcast_to(keep_y, (yp, bz))
    z_main = iz * bz + lane
    keep_z_main = jnp.broadcast_to(z_main < nz * bz - 1, (yp, bz))
    z_pack = iz * bz + jnp.where(spot < SEG // 2, spot - H, spot - SEG // 2 + bz - H)
    keep_z_pack = jnp.broadcast_to(
        jnp.logical_and(z_pack >= 0, z_pack < nz * bz - 1), (yp, bz)
    )
    start = ix * bx - off
    blocks = win + tiles

    def rows(ref, x, shift=0):
        return ref[base(x) + shift : base(x) + shift + yp]

    for x in range(blocks):
        value = rows(va, x) - scale * rows(ga, x)
        target[base(x) : base(x) + yp] = value

    for it in range(ITERS):
        now = target if it == 0 else extra
        held = target if it == 0 else current
        last = it == ITERS - 1
        for x in range(blocks):
            here = rows(now, x)
            b = base(x)
            ddy = jnp.where(keep_y, rows(now, x, 1) - here, 0.0)
            if x < win:
                g, k = x // tiles, x % tiles
                edge = roll(rows(now, win + k), bz - 1 - (SEG * g + SEG // 2 + H))
                after = jnp.where(lane == bz - 1, edge, roll(here, -1))
                ddz = jnp.where(keep_z_main, after - here, 0.0)
                if x == win - 1:
                    ddx = jnp.zeros_like(here)
                else:
                    ddx = rows(now, x + 1) - here
            else:
                k = x - win
                ddz = jnp.where(keep_z_pack, roll(here, -1) - here, 0.0)
                if k < tiles - 1:
                    after = rows(now, x + 1)
                else:
                    after = roll(rows(now, win), -SEG)
                ddx = jnp.where(tiles * group + k < win - 1, after - here, 0.0)
            px, py, pz = dual_step * ddx, dual_step * ddy, dual_step * ddz
            if it > 0:
                px, py, pz = rows(dx, x) + px, rows(dy, x) + py, rows(dz, x) + pz
            shrink = jnp.minimum(1.0, tv_weight * lax.rsqrt(px * px + py * py + pz * pz))
            dx[b : b + yp] = px * shrink
            dy[b : b + yp] = py * shrink
            dz[b : b + yp] = pz * shrink
        for x in range(win if last else blocks):
            b = base(x)
            qx, qy, qz = rows(dx, x), rows(dy, x), rows(dz, x)
            spread = qy - rows(dy, x, -1)
            if x < win:
                g, k = x // tiles, x % tiles
                edge = roll(rows(dz, win + k), -(SEG * g + H - 1))
                spread = spread + (qz - jnp.where(lane == 0, edge, roll(qz, 1)))
                spread = spread + (qx if x == 0 else qx - rows(dx, x - 1))
            else:
                k = x - win
                spread = spread + (qz - roll(qz, 1))
                before = rows(dx, x - 1) if k > 0 else roll(rows(dx, blocks - 1), SEG)
                spread = spread + (qx - before)
            old = rows(held, x)
            new = (old + primal_step * (spread + rows(target, x))) * (1.0 / (1.0 + primal_step))
            if last:
                result[x] = new[H : H + by]
            else:
                current[b : b + yp] = new
                extra[b : b + yp] = 2.0 * new - old

    m_out = pltpu.make_async_copy(result.at[pl.ds(off, bx)], model_out, out_sem.at[1])
    m_out.start()
    g_out.wait()
    m_out.wait()


def shards(partials, code_bits, group_map, velocity):
    slots = partials.shape[0]
    bx, by, bz = velocity.shape
    nx, ny, nz = (lax.axis_size(a) for a in ("gx", "gy", "gz"))
    dims = (nx, ny, nz, slots, bx, by, bz)
    win, tiles, yp, flat = geometry(dims)
    strip = -(-(win * H + 5) // 8) * 8
    diag = -(-(tiles * H + 5) // 8) * 8
    f32 = functools.partial(pltpu.VMEM, dtype=jnp.float32)
    per = bx * by // 8
    third = -(-per // 3)
    dma = pltpu.SemaphoreType.DMA
    anywhere = pl.BlockSpec(memory_space=pl.ANY)
    near = pl.BlockSpec(memory_space=pltpu.VMEM)
    block = jax.ShapeDtypeStruct(velocity.shape, jnp.float32)
    handed = (f32((flat, bz)), f32((flat, bz)), f32((win, by, bz)), f32((1, bz)))
    assembled = pl.pallas_call(
        functools.partial(kernel, dims),
        out_shape=handed,
        in_specs=[pl.BlockSpec(memory_space=pltpu.HBM)] * 4,
        out_specs=(near,) * 4,
        scratch_shapes=[
            pltpu.SMEM(code_bits.shape, jnp.int32),
            pltpu.SMEM(group_map.shape, jnp.int32),
            f32(partials.shape),
            f32((nx * per, 8, bz)),
            f32((win, by, bz)),
            f32((3, 4, third, 8, bz)),
            f32((3, 2, third, 8, bz)),
            f32((3, third, 8, bz)),
            f32((3, 2, third, 8, bz)),
            f32((3, third, 8, bz)),
            f32((2, 2, strip, bz)),
            f32((2, 2, strip, bz)),
            f32((2, tiles, by, bz)),
            f32((2, 2, tiles, by, bz)),
            f32((2, 2, diag, bz)),
            f32((4, 2, diag, bz)),
            f32((2, yp + 8, bz)),
            f32((4 * nz, 1, bz)),
            f32((2 * ny, 1, bz)),
            dma((3,)),
            dma((nx,)),
            dma((3, 4)),
            dma((3, 4)),
            dma((3, 2)),
            dma((3, 2)),
            dma((3,)),
            dma((3,)),
            dma((2, 2)),
            dma((2, 2)),
            dma((2, 8)),
            dma((2, 8)),
            dma,
            dma,
            dma,
            dma,
        ],
        compiler_params=pltpu.CompilerParams(
            collective_id=0, has_side_effects=True
        ),
    )(partials, code_bits, group_map, velocity)
    return pl.pallas_call(
        functools.partial(proximal, dims),
        out_shape=(block, block),
        in_specs=[near] * 4,
        out_specs=(anywhere, anywhere),
        scratch_shapes=[f32((flat, bz))] * 6 + [f32((win, by, bz)), dma((2,))],
        compiler_params=pltpu.CompilerParams(vmem_limit_bytes=32 * 2**20),
    )(*assembled)


def solution(mesh):
    placed = (P("gx", None, "gy", "gz"), P(), P(), P("gx", "gy", "gz"))
    return jax.shard_map(
        shards,
        mesh=mesh,
        in_specs=placed,
        out_specs=(P("gx", "gy", "gz"), P("gx", "gy", "gz")),
        check_vma=False,
    )
```

```python
import functools

import jax
import jax.numpy as jnp
from jax import lax
from jax.experimental import pallas as pl
from jax.experimental.pallas import tpu as pltpu
from jax.sharding import PartitionSpec as P

ITERS = 3
H = ITERS
SEG = 16
PARTS = ((2, 6, 1), (6, 1, 2), (1, 2, 6))
LOAD_ORDER = (5, 4, 7, 3, 2, 6, 1, 0)

step_length = 0.5
tv_weight = 0.2
dual_step = 0.28
primal_step = 0.28
MESH = pl.DeviceIdType.MESH


def geometry(dims):
    nx, ny, nz, slots, bx, by, bz = dims
    win = bx + H * min(2, nx - 1)
    tiles = -(-win // (bz // SEG))
    yp = -(-(by + 2 * H) // 8) * 8
    return win, tiles, yp, 16 + (win + tiles) * yp


def own_offset(nx, bx, win, q):
    if nx == 1:
        return 0
    return jnp.where(q == 0, 0, jnp.where(q == nx - 1, win - bx, H))


def roll(value, shift):
    shift = shift % value.shape[1]
    return value if shift == 0 else pltpu.roll(value, shift, 1)


def xor_masks(ix):
    two = ix + 2 - 4 * lax.rem(lax.div(ix, 2), 2)
    six = 6 - 2 * lax.div(ix, 2) + lax.rem(ix, 2)
    four = lax.rem(ix + 4, 8)
    flip = lambda q: q + 1 - 2 * lax.rem(q, 2)
    return {
        0: ix, 1: flip(ix), 2: two, 3: flip(two),
        4: four, 5: flip(four), 6: six, 7: flip(six),
    }


def kernel(
    dims,
    partials,
    code_bits,
    group_map,
    velocity,
    va,
    ga,
    gw,
    scale_out,
    bits,
    gmap,
    part,
    psum,
    vw,
    r1,
    r2,
    r3,
    s2,
    s3,
    ys,
    yr,
    ss,
    zr,
    ds,
    dr,
    za,
    ara,
    arb,
    in_sem,
    part_sem,
    rs_send,
    rs_recv,
    xs_sem,
    xr_sem,
    hs_sem,
    hr_sem,
    as_sem,
    ar_sem,
    bs_sem,
    br_sem,
    round_sem,
):
    nx, ny, nz, slots, bx, by, bz = dims
    win, tiles, yp, flat = geometry(dims)
    groups = bz // SEG
    ix, iy, iz = lax.axis_index("gx"), lax.axis_index("gy"), lax.axis_index("gz")
    xi, zl = lax.div(ix, 2), lax.rem(ix, 2)
    offset = functools.partial(own_offset, nx, bx, win)
    off = offset(ix)
    block = xor_masks(ix)
    per = bx * by // 8

    in_copies = [
        pltpu.make_async_copy(code_bits, bits, in_sem.at[0]),
        pltpu.make_async_copy(group_map, gmap, in_sem.at[1]),
    ]
    v_copy = pltpu.make_async_copy(velocity, vw.at[pl.ds(off, bx)], in_sem.at[2])
    for c in in_copies:
        c.start()
    part_copies = {}
    for mask in LOAD_ORDER:
        where = pl.ds(block[mask] * bx, bx)
        part_copies[mask] = pltpu.make_async_copy(
            partials.at[:, where], part.at[:, where], part_sem.at[mask]
        )
        part_copies[mask].start()
    v_copy.start()

    barrier = pltpu.get_barrier_semaphore()

    def at(x=None, y=None, z=None):
        return (ix if x is None else x, iy if y is None else y, iz if z is None else z)

    def notify(sem, device):
        pl.semaphore_signal(sem, inc=1, device_id=device, device_id_type=MESH)

    for buffer in (yr, zr, dr):
        buffer[...] = jnp.zeros_like(buffer)

    ring = lambda d, n: min(d, n - d)
    plane = [(dx, dz) for dx in range(4) for dz in range(nz) if dx or dz]
    plane.sort(key=lambda p: -(ring(p[0], 4) + ring(p[1], nz)))
    stack = [(dl, dy) for dl in range(2) for dy in range(ny) if dl or dy]
    stack.sort(key=lambda p: -(p[0] + 2 * ring(p[1] // 2, max(ny // 2, 1)) + p[1] % 2))

    def plane_device(dx, dz):
        return at(x=2 * lax.rem(xi + dx, 4) + zl, z=lax.rem(iz + dz, nz))

    def stack_device(dl, dy):
        return at(x=2 * xi + lax.rem(zl + dl, 2), y=lax.rem(iy + dy, ny))

    has = {
        "y-": iy > 0,
        "y+": iy < ny - 1,
        "z-": iz > 0,
        "z+": iz < nz - 1,
    }
    near = {
        "y-": at(y=iy - 1),
        "y+": at(y=iy + 1),
        "z-": at(z=iz - 1),
        "z+": at(z=iz + 1),
    }
    both = lambda a, b: jnp.logical_and(has[a], has[b])
    ring_x = (at(x=block[2]), at(x=block[6]))
    ring_y = (at(z=lax.rem(iz + 1, nz)), at(z=lax.rem(iz + nz - 1, nz)))
    beyond = lax.rem(iy + ny + 4 * zl - 2, ny)
    around = ring_x + ring_y + (
        at(x=block[1]),
        at(x=block[1], y=beyond),
        at(y=iy + 1 - 2 * lax.rem(iy, 2)),
    )

    def greet(sem):
        for device in around:
            notify(sem, device)

    def hear(sem):
        pl.semaphore_wait(sem, len(around))

    greet(barrier)

    for buffer in (za, va, ga):
        buffer[...] = jnp.zeros_like(buffer)

    def x_halo(buffer, f, side):
        q = ix + 1 if side == 0 else ix - 1
        src = off + bx - H if side == 0 else off
        dst = offset(q) - H if side == 0 else offset(q) + bx
        return pltpu.make_async_remote_copy(
            src_ref=buffer.at[pl.ds(src, H)],
            dst_ref=buffer.at[pl.ds(dst, H)],
            send_sem=xs_sem.at[f, side],
            recv_sem=xr_sem.at[f, side],
            device_id=at(x=q),
            device_id_type=MESH,
        )

    def x_send(buffer, f):
        pl.when(ix < nx - 1)(x_halo(buffer, f, 0).start)
        pl.when(ix > 0)(x_halo(buffer, f, 1).start)

    def x_arrive(buffer, f):
        for side in range(2):
            zone = buffer.at[pl.ds(off - H if side == 0 else off + bx, H)]
            arrived = pltpu.make_async_copy(zone, zone, xr_sem.at[f, side])
            pl.when(ix > 0 if side == 0 else ix < nx - 1)(arrived.wait)

    for c in in_copies:
        c.wait()
    codes = [gmap[ix * slots + s] for s in range(slots)]

    def reduce_block(mask):
        part_copies[mask].wait()
        first = block[mask] * bx

        def one(r, carry):
            row = first + r
            acc = None
            for s in range(slots):
                sign = (2 * bits[codes[s], row] - 1).astype(jnp.float32)
                term = sign * part[s, row]
                acc = term if acc is None else acc + term
            for h in range(by // 8):
                psum[row * (by // 8) + h] = acc[8 * h : 8 * h + 8]
            return carry

        lax.fori_loop(0, bx, one, 0, unroll=4)

    cuts = [per * k // 3 for k in range(4)]
    sizes = [cuts[k + 1] - cuts[k] for k in range(3)]
    lots = [(0, 0), (0, 1), (1, None), (2, None), (3, None)]

    def piece(k, lot):
        middle = (sizes[k] + 1) // 2
        return {0: (0, middle), 1: (middle, sizes[k]), None: (0, sizes[k])}[lot[1]]

    def mine(mask, k, lot):
        low, high = piece(k, lot)
        return pl.ds(block[mask] * per + cuts[k] + low, high - low)

    def kept(k, m):
        a, b, c = PARTS[k]
        return (b ^ c, b, c, 0)[m]

    def hop(k, step, src, dst, n):
        return pltpu.make_async_remote_copy(
            src_ref=src,
            dst_ref=dst,
            send_sem=rs_send.at[k, n],
            recv_sem=rs_recv.at[k, n],
            device_id=at(x=block[PARTS[k][step]]),
            device_id_type=MESH,
        )

    def first_hop(k, lot):
        low, high = piece(k, lot)
        src = psum.at[mine(PARTS[k][0] ^ kept(k, lot[0]), k, lot)]
        return hop(k, 0, src, r1.at[k, lot[0], low:high], lots.index(lot))

    def second_hop(k, lot):
        low, high = piece(k, lot)
        return hop(k, 1, s2.at[k, lot[0], low:high], r2.at[k, lot[0], low:high], 5 + lots.index(lot))

    def third_hop(k, half):
        low, high = piece(k, (0, half))
        return hop(k, 2, s3.at[k, low:high], r3.at[k, low:high], 8 + half)

    reduced = set()

    def send_first(lot):
        for k in range(3):
            mask = PARTS[k][0] ^ kept(k, lot[0])
            if mask not in reduced:
                reduced.add(mask)
                reduce_block(mask)
            first_hop(k, lot).start()

    def forward(lot):
        for k in range(3):
            first_hop(k, lot).wait_recv()
            low, high = piece(k, lot)
            m = lot[0]
            s2[k, m, low:high] = psum[mine(kept(k, m), k, lot)] + r1[k, m, low:high]
            second_hop(k, lot).start()

    reduced.add(5)
    reduce_block(5)
    hear(barrier)
    for lot in lots[:4]:
        send_first(lot)
    greet(round_sem.at[0])
    for mask in LOAD_ORDER:
        if mask not in reduced:
            reduced.add(mask)
            reduce_block(mask)
    hear(round_sem.at[0])
    greet(round_sem.at[1])
    forward(lots[0])
    forward(lots[1])
    send_first(lots[4])
    hear(round_sem.at[1])
    greet(round_sem.at[2])
    forward(lots[2])
    hear(round_sem.at[2])
    greet(round_sem.at[3])
    for half in range(2):
        for k in range(3):
            if half == 0:
                first_hop(k, lots[3]).wait_recv()
            second_hop(k, lots[half]).wait_recv()
            low, high = piece(k, (0, half))
            here = pl.ds(block[kept(k, 2)] * per + cuts[k] + low, high - low)
            s3[k, low:high] = psum[here] + r1[k, 2, low:high] + r2[k, 0, low:high]
            third_hop(k, half).start()
    v_copy.wait()
    x_send(vw, 0)
    hear(round_sem.at[3])

    lane = lax.broadcasted_iota(jnp.int32, (1, bz), 1)
    group = lane // SEG
    spot = lax.rem(lane, SEG)

    def pack(read, k):
        acc = None
        for g in range(groups):
            x = tiles * g + k
            if x >= win:
                continue
            moved = roll(read(x), H + SEG * g)
            acc = moved if acc is None else jnp.where(group == g, moved, acc)
        return acc

    def prepare(f, field):
        for x in range(win):
            tile = field[x]
            ys[0, f, x * H : x * H + H] = tile[by - H : by]
            ys[1, f, x * H : x * H + H] = tile[0:H]
        for k in range(tiles):
            tile = pack(lambda x: field[x], k)
            ss[f, k] = tile
            ds[0, f, k * H : k * H + H] = tile[by - H : by]
            ds[1, f, k * H : k * H + H] = tile[0:H]

    def exchange(f):
        def send(src, dst, n, device):
            return pltpu.make_async_remote_copy(
                src_ref=src.at[f],
                dst_ref=dst.at[f],
                send_sem=hs_sem.at[f, n],
                recv_sem=hr_sem.at[f, n],
                device_id=device,
                device_id_type=MESH,
            )

        up, down = ds.at[0], ds.at[1]
        pp, pm = both("y+", "z+"), both("y+", "z-")
        mp, mm = both("y-", "z+"), both("y-", "z-")
        return [
            (send(ys.at[0], yr.at[0], 0, near["y+"]), has["y+"], has["y-"]),
            (send(ys.at[1], yr.at[1], 1, near["y-"]), has["y-"], has["y+"]),
            (send(ss, zr.at[0], 2, near["z+"]), has["z+"], has["z-"]),
            (send(ss, zr.at[1], 3, near["z-"]), has["z-"], has["z+"]),
            (send(up, dr.at[0], 4, at(y=iy + 1, z=iz + 1)), pp, mm),
            (send(up, dr.at[1], 5, at(y=iy + 1, z=iz - 1)), pm, mp),
            (send(down, dr.at[2], 6, at(y=iy - 1, z=iz + 1)), mp, pm),
            (send(down, dr.at[3], 7, at(y=iy - 1, z=iz - 1)), mm, pp),
        ]

    def send_all(f):
        for copy, sends, _ in exchange(f):
            pl.when(sends)(copy.start)

    def receive_all(f):
        for copy, _, receives in exchange(f):
            pl.when(receives)(copy.wait_recv)

    front = 8

    def base(x):
        return front + x * yp

    def assemble(f, field, whole):
        for x in range(win):
            b = base(x)
            whole[b + H : b + H + by] = field[x]
            whole[b : b + H] = yr[0, f, x * H : x * H + H]
            whole[b + H + by : b + 2 * H + by] = yr[1, f, x * H : x * H + H]
        for k in range(tiles):
            for z in range(2):
                za[z, H : H + by] = zr[z, f, k]
                za[z, 0:H] = dr[z, f, k * H : k * H + H]
                za[z, H + by : 2 * H + by] = dr[2 + z, f, k * H : k * H + H]
            left = za[0, 0:yp]
            mine = pack(lambda x: whole[base(x) : base(x) + yp], k)
            right = roll(za[1, 0:yp], SEG // 2)
            b = base(win + k)
            whole[b : b + yp] = jnp.where(
                spot < H,
                left,
                jnp.where(
                    spot < SEG // 2,
                    mine,
                    jnp.where(spot < SEG // 2 + H, roll(mine, SEG // 2), right),
                ),
            )

    squares = jnp.zeros((8, bz), jnp.float32)
    for k in range(3):
        first_hop(k, lots[4]).wait_recv()
        second_hop(k, lots[2]).wait_recv()
        for half in range(2):
            third_hop(k, half).wait_recv()
        for j in range(cuts[k], cuts[k + 1]):
            n = j - cuts[k]
            value = psum[ix * per + j] + r1[k, 3, n] + (r2[k, 1, n] + r3[k, n])
            r, h = divmod(j, by // 8)
            gw[off + r, 8 * h : 8 * h + 8] = value
            squares = squares + value * value

    def spread(buffer, me, peers, device, send_sem, recv_sem):
        for p in peers:
            pltpu.make_async_remote_copy(
                src_ref=buffer.at[me],
                dst_ref=buffer.at[me],
                send_sem=send_sem,
                recv_sem=recv_sem,
                device_id=device(*p),
                device_id_type=MESH,
            ).start()

    def drain(buffer, peers, sem):
        many = buffer.at[pl.ds(0, len(peers))]
        pltpu.make_async_copy(many, many, sem).wait()

    me_a = xi * nz + iz
    ara[me_a] = jnp.sum(squares, axis=0, keepdims=True)
    spread(ara, me_a, plane, plane_device, as_sem, ar_sem)
    x_send(gw, 1)
    x_arrive(vw, 0)
    prepare(0, vw)
    send_all(0)
    x_arrive(gw, 1)
    prepare(1, gw)
    send_all(1)

    drain(ara, plane, ar_sem)
    me_b = zl * ny + iy
    arb[me_b] = jnp.sum(ara[...], axis=0)
    spread(arb, me_b, stack, stack_device, bs_sem, br_sem)

    for k in range(3):
        for lot in lots:
            first_hop(k, lot).wait_send()
        for lot in lots[:3]:
            second_hop(k, lot).wait_send()
        for half in range(2):
            third_hop(k, half).wait_send()
    receive_all(0)
    assemble(0, vw, va)
    receive_all(1)
    assemble(1, gw, ga)
    drain(ara, plane, as_sem)
    for f, buffer in ((0, vw), (1, gw)):
        pl.when(ix < nx - 1)(x_halo(buffer, f, 0).wait_send)
        pl.when(ix > 0)(x_halo(buffer, f, 1).wait_send)
        for copy, sends, _ in exchange(f):
            pl.when(sends)(copy.wait_send)

    drain(arb, stack, br_sem)
    square_sum = jnp.sum(jnp.sum(arb[...], axis=0), axis=1, keepdims=True)
    cells = nx * ny * nz * bx * by * bz
    scale = step_length * lax.rsqrt(square_sum / cells + 1.0)
    scale_out[...] = jnp.broadcast_to(scale, scale_out.shape)
    drain(arb, stack, bs_sem)


def proximal(
    dims,
    va,
    ga,
    gw,
    scale_in,
    gradient_out,
    model_out,
    target,
    current,
    extra,
    dx,
    dy,
    dz,
    result,
    out_sem,
):
    nx, ny, nz, slots, bx, by, bz = dims
    win, tiles, yp, flat = geometry(dims)
    ix, iy, iz = lax.axis_index("gx"), lax.axis_index("gy"), lax.axis_index("gz")
    off = own_offset(nx, bx, win, ix)
    g_out = pltpu.make_async_copy(gw.at[pl.ds(off, bx)], gradient_out, out_sem.at[0])
    g_out.start()
    front = 8

    def base(x):
        return front + x * yp

    edge_rows = jnp.zeros((front, bz), jnp.float32)
    dy[0:front] = edge_rows
    target[flat - front : flat] = edge_rows
    extra[flat - front : flat] = edge_rows
    scale = scale_in[...]
    lane = lax.broadcasted_iota(jnp.int32, (1, bz), 1)
    group = lane // SEG
    spot = lax.rem(lane, SEG)
    y_at = iy * by - H + lax.broadcasted_iota(jnp.int32, (yp, 1), 0)
    keep_y = jnp.logical_and(y_at >= 0, y_at < ny * by - 1)
    keep_y = jnp.broadcast_to(keep_y, (yp, bz))
    z_main = iz * bz + lane
    keep_z_main = jnp.broadcast_to(z_main < nz * bz - 1, (yp, bz))
    z_pack = iz * bz + jnp.where(spot < SEG // 2, spot - H, spot - SEG // 2 + bz - H)
    keep_z_pack = jnp.broadcast_to(
        jnp.logical_and(z_pack >= 0, z_pack < nz * bz - 1), (yp, bz)
    )
    start = ix * bx - off
    blocks = win + tiles

    def rows(ref, x, shift=0):
        return ref[base(x) + shift : base(x) + shift + yp]

    for x in range(blocks):
        value = rows(va, x) - scale * rows(ga, x)
        target[base(x) : base(x) + yp] = value

    for it in range(ITERS):
        now = target if it == 0 else extra
        held = target if it == 0 else current
        last = it == ITERS - 1
        for x in range(blocks):
            here = rows(now, x)
            b = base(x)
            ddy = jnp.where(keep_y, rows(now, x, 1) - here, 0.0)
            if x < win:
                g, k = x // tiles, x % tiles
                edge = roll(rows(now, win + k), bz - 1 - (SEG * g + SEG // 2 + H))
                after = jnp.where(lane == bz - 1, edge, roll(here, -1))
                ddz = jnp.where(keep_z_main, after - here, 0.0)
                if x == win - 1:
                    ddx = jnp.zeros_like(here)
                else:
                    ddx = rows(now, x + 1) - here
            else:
                k = x - win
                ddz = jnp.where(keep_z_pack, roll(here, -1) - here, 0.0)
                if k < tiles - 1:
                    after = rows(now, x + 1)
                else:
                    after = roll(rows(now, win), -SEG)
                ddx = jnp.where(tiles * group + k < win - 1, after - here, 0.0)
            px, py, pz = dual_step * ddx, dual_step * ddy, dual_step * ddz
            if it > 0:
                px, py, pz = rows(dx, x) + px, rows(dy, x) + py, rows(dz, x) + pz
            shrink = jnp.minimum(1.0, tv_weight * lax.rsqrt(px * px + py * py + pz * pz))
            dx[b : b + yp] = px * shrink
            dy[b : b + yp] = py * shrink
            dz[b : b + yp] = pz * shrink
        for x in range(win if last else blocks):
            b = base(x)
            qx, qy, qz = rows(dx, x), rows(dy, x), rows(dz, x)
            spread = qy - rows(dy, x, -1)
            if x < win:
                g, k = x // tiles, x % tiles
                edge = roll(rows(dz, win + k), -(SEG * g + H - 1))
                spread = spread + (qz - jnp.where(lane == 0, edge, roll(qz, 1)))
                spread = spread + (qx if x == 0 else qx - rows(dx, x - 1))
            else:
                k = x - win
                spread = spread + (qz - roll(qz, 1))
                before = rows(dx, x - 1) if k > 0 else roll(rows(dx, blocks - 1), SEG)
                spread = spread + (qx - before)
            old = rows(held, x)
            new = (old + primal_step * (spread + rows(target, x))) * (1.0 / (1.0 + primal_step))
            if last:
                result[x] = new[H : H + by]
            else:
                current[b : b + yp] = new
                extra[b : b + yp] = 2.0 * new - old

    m_out = pltpu.make_async_copy(result.at[pl.ds(off, bx)], model_out, out_sem.at[1])
    m_out.start()
    g_out.wait()
    m_out.wait()


def shards(partials, code_bits, group_map, velocity):
    slots = partials.shape[0]
    bx, by, bz = velocity.shape
    nx, ny, nz = (lax.axis_size(a) for a in ("gx", "gy", "gz"))
    dims = (nx, ny, nz, slots, bx, by, bz)
    win, tiles, yp, flat = geometry(dims)
    strip = -(-(win * H + 5) // 8) * 8
    diag = -(-(tiles * H + 5) // 8) * 8
    f32 = functools.partial(pltpu.VMEM, dtype=jnp.float32)
    per = bx * by // 8
    third = -(-per // 3)
    dma = pltpu.SemaphoreType.DMA
    anywhere = pl.BlockSpec(memory_space=pl.ANY)
    near = pl.BlockSpec(memory_space=pltpu.VMEM)
    block = jax.ShapeDtypeStruct(velocity.shape, jnp.float32)
    handed = (f32((flat, bz)), f32((flat, bz)), f32((win, by, bz)), f32((1, bz)))
    assembled = pl.pallas_call(
        functools.partial(kernel, dims),
        out_shape=handed,
        in_specs=[pl.BlockSpec(memory_space=pltpu.HBM)] * 4,
        out_specs=(near,) * 4,
        scratch_shapes=[
            pltpu.SMEM(code_bits.shape, jnp.int32),
            pltpu.SMEM(group_map.shape, jnp.int32),
            f32(partials.shape),
            f32((nx * per, 8, bz)),
            f32((win, by, bz)),
            f32((3, 4, third, 8, bz)),
            f32((3, 2, third, 8, bz)),
            f32((3, third, 8, bz)),
            f32((3, 2, third, 8, bz)),
            f32((3, third, 8, bz)),
            f32((2, 2, strip, bz)),
            f32((2, 2, strip, bz)),
            f32((2, tiles, by, bz)),
            f32((2, 2, tiles, by, bz)),
            f32((2, 2, diag, bz)),
            f32((4, 2, diag, bz)),
            f32((2, yp + 8, bz)),
            f32((4 * nz, 1, bz)),
            f32((2 * ny, 1, bz)),
            dma((3,)),
            dma((nx,)),
            dma((3, 10)),
            dma((3, 10)),
            dma((2, 2)),
            dma((2, 2)),
            dma((2, 8)),
            dma((2, 8)),
            dma,
            dma,
            dma,
            dma,
            pltpu.SemaphoreType.REGULAR((4,)),
        ],
        compiler_params=pltpu.CompilerParams(
            collective_id=0, has_side_effects=True
        ),
    )(partials, code_bits, group_map, velocity)
    return pl.pallas_call(
        functools.partial(proximal, dims),
        out_shape=(block, block),
        in_specs=[near] * 4,
        out_specs=(anywhere, anywhere),
        scratch_shapes=[f32((flat, bz))] * 6 + [f32((win, by, bz)), dma((2,))],
        compiler_params=pltpu.CompilerParams(vmem_limit_bytes=32 * 2**20),
    )(*assembled)


def solution(mesh):
    placed = (P("gx", None, "gy", "gz"), P(), P(), P("gx", "gy", "gz"))
    return jax.shard_map(
        shards,
        mesh=mesh,
        in_specs=placed,
        out_specs=(P("gx", "gy", "gz"), P("gx", "gy", "gz")),
        check_vma=False,
    )
```
